128 devices in a mesh: dp: 8 (over y, core), tensor: 16 (over x, z).
Axes of the slice: x: 4, y: 4, z: 4, core: 2. Of those that a mesh axis runs over, the one named last changes fastest.
Arguments:
- gradient: bfloat16 [4096, 14336], P('dp', 'tensor'), may hold values from -8000 to 8000
- block_owner: int32 [224], replicated, may hold values from 0 to 255, as said below
- tile_block: int32 [8, 112], replicated, may hold values from 0 to 223, as said below
- fast_weight: float32 [4096, 14336], P('dp', 'tensor'), may hold values from -6 to 6
- slow_flat: float32 [4096, 14336], P(('dp', 'tensor')), may hold values from -6 to 6
- left_stat: float32 [256, 512, 512], P(('dp', 'tensor')), may hold values from -6 to 6
- right_stat: float32 [256, 512, 512], P(('dp', 'tensor')), may hold values from -6 to 6
- left_basis: bfloat16 [256, 512, 512], P(('dp', 'tensor')), may hold values from -0.25 to 0.25
- right_basis: bfloat16 [256, 512, 512], P(('dp', 'tensor')), may hold values from -0.25 to 0.25
- first_moment: float32 [256, 512, 512], P(('dp', 'tensor')), may hold values from -3 to 3
- second_moment: float32 [256, 512, 512], P(('dp', 'tensor')), may hold values from 0.05 to 0.5
Outputs:
- fast_new: float32 [4096, 14336], P('dp', 'tensor')
- slow_new: float32 [4096, 14336], P(('dp', 'tensor'))
- left_new: float32 [256, 512, 512], P(('dp', 'tensor'))
- right_new: float32 [256, 512, 512], P(('dp', 'tensor'))
- moment_new: float32 [256, 512, 512], P(('dp', 'tensor'))
- second_new: float32 [256, 512, 512], P(('dp', 'tensor'))
The draws below stay inside these ranges and needn't reach their ends.
Inputs may be any that keep to these rules, and one draw needn't show every extreme that they name: `tile_block`: entry [r, g] is the number of the block that tile g of block row r (columns g * 128 to g * 128 + 127) belongs to, one of r * (28) to r * 28 + 14336 // 512 - 1. Each such block has 4 tiles, which lie in the columns of different tensor indices. In each row the tensor indices fall into groups of 4, and every block takes one tile from each member of one group. `block_owner`: entry b is the slot d * 2 + k of block b's owner, where d = (dp index) * (number of tensor indices) + (tensor index) and k is 0 or 1; the owner's dp index is the block's row. No slot is named twice, every device owns one or two blocks, and a device's two blocks come from different groups.
All inputs are finite; a program needn't handle non-finite values.
Results may differ from the reference program's by a relative error of at most 0.00095.
Values may be sent and summed in bfloat16 or wider, within the bound.
No kernel may reach another device: no remote copies, remote signals or barrier semaphores. Data moves between devices by JAX's collectives and lax.ppermute only.
A program may use at most 128 MiB of HBM per device.

```python
import math
import jax
import jax.numpy as jnp
from jax import lax

B = 512
TILE = 128
SHARD_COLS = 896
SLOTS = 2
ROWS = 4096
COLS = 14336
SLOT_TOTAL = 256
N_TENSOR = 16


def draw_gradient(key, part):
    noise_key, row_key, col_key = jax.random.split(key, 3)
    noise = jnp.clip(jax.random.normal(noise_key, (ROWS, COLS), jnp.float32), -6.0, 6.0)
    trend_rows = jnp.exp(math.log(3.0) * jnp.arange(ROWS, dtype=jnp.float32) / ROWS)
    trend_cols = jnp.exp(math.log(3.0) * jnp.arange(COLS, dtype=jnp.float32) / COLS)
    row_scale = jnp.exp(jax.random.uniform(row_key, (ROWS,), jnp.float32, 0.0, math.log(2.0)))
    col_scale = jnp.exp(jax.random.uniform(col_key, (COLS,), jnp.float32, 0.0, math.log(2.0)))
    rows_part = (row_scale * trend_rows)[:, None]
    cols_part = (col_scale * trend_cols)[None, :]
    return jnp.clip(noise * rows_part * cols_part, -8000.0, 8000.0).astype(jnp.bfloat16)


def layout_tables(key):
    base_key = jax.random.fold_in(key, 11)
    row_blocks = SHARD_COLS * N_TENSOR // B
    per_block = B // TILE
    shard_tiles = SHARD_COLS // TILE
    pair_count = row_blocks - N_TENSOR
    half_count = row_blocks // 2
    row_groups = ROWS // B

    def shuffle(tile_key):
        return jax.random.permutation(tile_key, shard_tiles)

    def one_row(row_key, block_row):
        subkeys = jax.random.split(row_key, 5)
        members = jax.random.permutation(subkeys[0], N_TENSOR)
        position = jnp.argsort(members).astype(jnp.int32)
        group_of = position // per_block
        tile_keys = jax.random.split(subkeys[1], N_TENSOR)
        tile_perm = jax.vmap(shuffle)(tile_keys).astype(jnp.int32)
        local_block = group_of[:, None] * shard_tiles + tile_perm
        relabel = jax.random.permutation(subkeys[2], row_blocks).astype(jnp.int32)
        tile_numbers = block_row * row_blocks + jnp.take(relabel, local_block.reshape(-1))
        owner_perm = jax.random.permutation(subkeys[3], N_TENSOR).astype(jnp.int32)
        flip_bits = jax.random.randint(subkeys[4], (row_blocks,), 0, 2).astype(jnp.int32)
        local_ids = jnp.arange(row_blocks, dtype=jnp.int32)
        second = local_ids >= half_count
        pair_pos = jnp.where(second, local_ids - half_count, local_ids)
        paired = pair_pos < pair_count
        single = jnp.where(second, half_count - pair_count + local_ids - half_count - pair_count, local_ids - pair_count)
        owner_index = jnp.where(paired, pair_pos, pair_count + single)
        device = jnp.take(owner_perm, owner_index)
        slot_bit = jnp.where(paired, (second.astype(jnp.int32) + jnp.take(flip_bits, pair_pos)) % 2, flip_bits)
        owner_value = (block_row * N_TENSOR + device) * SLOTS + slot_bit
        inverse = jnp.argsort(relabel).astype(jnp.int32)
        owners = jnp.take(owner_value, inverse)
        return (tile_numbers, owners)
    row_keys = jax.random.split(base_key, row_groups)
    tile_numbers, owners = jax.vmap(one_row)(row_keys, jnp.arange(row_groups, dtype=jnp.int32))
    return (tile_numbers.astype(jnp.int32), owners.reshape(-1).astype(jnp.int32))


def draw_tile_block(key, part):
    return layout_tables(key)[0]


def draw_block_owner(key, part):
    return layout_tables(key)[1]


def levels(stream_key, shape, shards, low, largest):
    gain = 1.0
    for dim, parts in shards:
        heights = jax.random.uniform(jax.random.fold_in(jax.random.fold_in(stream_key, 6), dim), (parts,), jnp.float32, low / len(shards), largest / len(shards))
        gain = gain * jnp.repeat(jnp.exp(heights), shape[dim] // parts).reshape((-1,) + (1,) * (len(shape) - 1 - dim))
    return gain


def gaussian(key, dims, spread, bound, pieces=(), kind=jnp.bfloat16):
    factor_of = levels(key, dims, pieces, -0.22, 0.18) if pieces else 1.0
    drawn = jax.random.normal(key, dims, jnp.float32) * spread * factor_of
    return jnp.minimum(jnp.maximum(drawn, -bound), bound).astype(kind)


def setup_inputs(seed: int = 0) -> dict:
    seeds = jax.random.split(jax.random.key(seed), 12)
    gradient = draw_gradient(jax.random.fold_in(seeds[11], 71), 0)
    block_owner = draw_block_owner(jax.random.fold_in(seeds[11], 71), 0)
    tile_block = draw_tile_block(jax.random.fold_in(seeds[11], 71), 0)
    fast_weight = gaussian(seeds[3], (ROWS, COLS), 1.0, 6.0, ((0, 8), (1, 16)), jnp.float32)
    slow_flat = gaussian(seeds[4], (ROWS, COLS), 1.0, 6.0, ((0, 128),), jnp.float32)
    left_stat = gaussian(seeds[5], (SLOT_TOTAL, B, B), 1.0, 6.0, ((0, 128),), jnp.float32)
    right_stat = gaussian(seeds[6], (SLOT_TOTAL, B, B), 1.0, 6.0, ((0, 128),), jnp.float32)
    left_basis = gaussian(seeds[7], (SLOT_TOTAL, B, B), B ** -0.5, 0.25, ((0, 128),))
    right_basis = gaussian(seeds[8], (SLOT_TOTAL, B, B), B ** -0.5, 0.25, ((0, 128),))
    first_moment = gaussian(seeds[9], (SLOT_TOTAL, B, B), 0.5, 3.0, ((0, 128),), jnp.float32)
    second_moment = jnp.clip(jnp.exp(math.log(0.5) - 2.3025851 * jax.random.uniform(seeds[10], (SLOT_TOTAL, B, B), jnp.float32) ** levels(seeds[10], (SLOT_TOTAL, B, B), ((0, 128),), -0.2, 0.2)), 0.05, 0.5)
    return dict(gradient=gradient, block_owner=block_owner, tile_block=tile_block, fast_weight=fast_weight, slow_flat=slow_flat, left_stat=left_stat, right_stat=right_stat, left_basis=left_basis, right_basis=right_basis, first_moment=first_moment, second_moment=second_moment)


BETA_STAT = 0.95
BETA_ONE = 0.9
BETA_TWO = 0.95
ADAM_EPS = 1e-08
STEP_RATE = 0.1
PULL_RATE = 0.5
CLIP_RMS = 0.5
HIGHEST = lax.Precision.HIGHEST

def soap_block(grad_block, factor, left_stat, right_stat, left_basis, right_basis, first_moment, second_moment):
    gram_left = jnp.dot(grad_block, grad_block.T, preferred_element_type=jnp.float32)
    gram_right = jnp.dot(grad_block.T, grad_block, preferred_element_type=jnp.float32)
    squared = factor * factor
    left_next = BETA_STAT * left_stat + (1.0 - BETA_STAT) * squared * gram_left
    right_next = BETA_STAT * right_stat + (1.0 - BETA_STAT) * squared * gram_right
    left_wide = left_basis.astype(jnp.float32)
    right_wide = right_basis.astype(jnp.float32)
    half_rotated = jnp.dot(left_basis.T, grad_block, preferred_element_type=jnp.float32)
    rotated = factor * jnp.dot(half_rotated, right_wide, precision=HIGHEST)
    moment_next = BETA_ONE * first_moment + (1.0 - BETA_ONE) * factor * grad_block.astype(jnp.float32)
    second_next = BETA_TWO * second_moment + (1.0 - BETA_TWO) * rotated * rotated
    moment_turned = jnp.dot(jnp.dot(left_wide.T, moment_next, precision=HIGHEST), right_wide, precision=HIGHEST)
    direction = moment_turned / (jnp.sqrt(second_next) + ADAM_EPS)
    update = jnp.dot(jnp.dot(left_wide, direction, precision=HIGHEST), right_wide.T, precision=HIGHEST)
    return (left_next, right_next, moment_next, second_next, update.astype(jnp.bfloat16))

def reference(gradient, block_owner, tile_block, fast_weight, slow_flat, left_stat, right_stat, left_basis, right_basis, first_moment, second_moment):
    row_count, col_count = gradient.shape
    block_size = left_stat.shape[1]
    row_groups = row_count // block_size
    tile_count = tile_block.shape[1]
    tile_width = col_count // tile_count
    per_block = block_size // tile_width
    row_blocks = col_count // block_size
    wide_grad = gradient.astype(jnp.float32)
    factor = CLIP_RMS / jnp.sqrt(jnp.mean(wide_grad * wide_grad) + 1e-06)
    tile_ids = jnp.arange(tile_count, dtype=jnp.int32)
    tile_order = jnp.argsort(tile_block.astype(jnp.int32) * tile_count + tile_ids[None, :], axis=1).astype(jnp.int32)
    block_tiles = tile_order.reshape(row_groups * row_blocks, per_block)
    tiled_grad = gradient.reshape(row_groups, block_size, tile_count, tile_width)

    def one_block(block_index):
        block_row = block_index // row_blocks
        row_tiles = lax.dynamic_index_in_dim(tiled_grad, block_row, 0, keepdims=False)
        picked = lax.dynamic_index_in_dim(block_tiles, block_index, 0, keepdims=False)
        grad_block = jnp.take(row_tiles, picked, axis=1).reshape(block_size, block_size)
        owner_slot = block_owner[block_index]

        def choose(states):
            return lax.dynamic_index_in_dim(states, owner_slot, 0, keepdims=False)
        return soap_block(grad_block, factor, choose(left_stat), choose(right_stat), choose(left_basis), choose(right_basis), choose(first_moment), choose(second_moment))
    results = lax.map(one_block, jnp.arange(block_owner.shape[0], dtype=jnp.int32))
    left_new = left_stat.at[block_owner].set(results[0])
    right_new = right_stat.at[block_owner].set(results[1])
    moment_new = first_moment.at[block_owner].set(results[2])
    second_new = second_moment.at[block_owner].set(results[3])
    update = results[4].reshape(row_groups, row_blocks, block_size, per_block, tile_width)
    update = update.transpose(0, 1, 3, 2, 4).reshape(row_groups, tile_count, block_size, tile_width)
    placed = jnp.zeros_like(update)
    placed = placed.at[jnp.arange(row_groups, dtype=jnp.int32)[:, None], tile_order].set(update)
    update = placed.transpose(0, 2, 1, 3).reshape(row_count, col_count)
    fast_new = fast_weight - STEP_RATE * update.astype(jnp.float32)
    slow_new = slow_flat + PULL_RATE * (fast_new - slow_flat)
    return (fast_new, slow_new, left_new, right_new, moment_new, second_new)
```

```python
import functools

import jax
import jax.numpy as jnp
from jax import lax
from jax.experimental import pallas as pl
from jax.experimental.pallas import tpu as pltpu
from jax.sharding import Mesh
from jax.sharding import PartitionSpec as P

TENSOR = ("tensor_0", "tensor_1")
DP = ("dp_0", "dp_1")
DP_TENSOR = ("dp_0", "dp_1", "tensor_0", "tensor_1")

BETA_STAT = 0.95
BETA_ONE = 0.9
BETA_TWO = 0.95
ADAM_EPS = 1e-08
STEP_RATE = 0.1
PULL_RATE = 0.5
CLIP_RMS = 0.5

F32 = jnp.float32
BF16 = jnp.bfloat16
TILE = 128
MIB = 1 << 20


def dot(a, b, dims=((1,), (0,))):
    return lax.dot_general(a, b, (dims, ((), ())), preferred_element_type=F32)


def halves(x):
    high = x.astype(BF16)
    return high, (x - high.astype(F32)).astype(BF16)


def params(mib, **kw):
    return pltpu.CompilerParams(vmem_limit_bytes=mib * MIB, **kw)


SMEM = pl.BlockSpec(memory_space=pltpu.SMEM)
ANY = pl.BlockSpec(memory_space=pl.ANY)


def pack_tiles(gradient, tile_block, block_owner, tensor_size):
    rows, cols = gradient.shape
    tiles = cols // TILE

    def body(tb, owner, grad, out, sems):
        row = lax.axis_index(DP)
        column = lax.axis_index(TENSOR)
        copies = []
        for i in range(tiles):
            slot = owner[tb[row, column * tiles + i]]
            target = (slot >> 1) & (tensor_size - 1)
            copy = pltpu.make_async_copy(
                grad.at[:, pl.ds(i * TILE, TILE)], out.at[target], sems.at[i]
            )
            copy.start()
            copies.append(copy)
        for copy in copies:
            copy.wait()

    return pl.pallas_call(
        body,
        out_shape=jax.ShapeDtypeStruct((tensor_size, rows, TILE), BF16),
        in_specs=[SMEM, SMEM, ANY],
        out_specs=ANY,
        scratch_shapes=[pltpu.SemaphoreType.DMA((tiles,))],
        compiler_params=params(1),
        name="pack",
    )(tile_block, block_owner, gradient)


def route_tables(tile_block, block_owner, tensor_size, shard_tiles, row_blocks, per_block):
    tile_count = tile_block.shape[1]

    def body(tb, owner, out, count):
        row = lax.axis_index(DP)
        mine = row * tensor_size + lax.axis_index(TENSOR)

        def clear(i, c):
            count[i] = 0
            return c

        lax.fori_loop(0, row_blocks, clear, 0)
        for i in range(tile_count, tile_count + 16):
            out[i] = 0

        def step(g, c):
            block = tb[row, g]
            local = block - row * row_blocks
            j = count[local]
            count[local] = j + 1
            slot = owner[block]
            out[g] = (((slot >> 1) & (tensor_size - 1)) * 2 + (slot & 1)) * per_block + j

            @pl.when((slot >> 1) == mine)
            def _():
                out[tile_count + (slot & 1) * per_block + j] = g // shard_tiles
                out[tile_count + 8 + (slot & 1)] = 1

            return c

        lax.fori_loop(0, tile_count, step, 0)

    return pl.pallas_call(
        body,
        out_shape=jax.ShapeDtypeStruct((128,), jnp.int32),
        in_specs=[SMEM, SMEM],
        out_specs=SMEM,
        scratch_shapes=[pltpu.SMEM((row_blocks,), jnp.int32)],
        compiler_params=params(1),
        name="tables",
    )(tile_block, block_owner)


def slot_spec(size):
    return pl.BlockSpec((1, size, size), lambda k, *_: (k, 0, 0))


def turn_moment(left, right, moment):
    slots, size, _ = left.shape

    def body(left_ref, right_ref, moment_ref, out, flipped):
        left_t = left_ref[0].T
        flipped[0] = left_t
        high, low = halves(moment_ref[0])
        half = dot(left_t, high) + dot(left_t, low)
        high, low = halves(half)
        out[0] = dot(high, right_ref[0]) + dot(low, right_ref[0])

    return pl.pallas_call(
        body,
        grid=(slots,),
        out_shape=(
            jax.ShapeDtypeStruct((slots, size, size), F32),
            jax.ShapeDtypeStruct((slots, size, size), BF16),
        ),
        in_specs=[slot_spec(size)] * 3,
        out_specs=(slot_spec(size), slot_spec(size)),
        compiler_params=params(20),
        name="turn_moment",
    )(left, right, moment)


def tile_specs(size, per_block, base):
    def spec(j):
        return pl.BlockSpec((1, size, TILE), lambda k, tab: (tab[base + k * per_block + j], 0, 0))

    return [spec(j) for j in range(per_block)]


def main_step(tables, factor, arrived, turned, left_t, left, right, second, base):
    slots, size, _ = left.shape
    per_block = size // TILE
    peers = arrived.shape[0]
    rows = size // peers

    def body(tab, factor_ref, *refs):
        tiles = refs[:per_block]
        turned_ref, left_t_ref, left_ref, right_ref, second_ref, second_out, send = refs[per_block:]
        k = pl.program_id(0)
        scale = factor_ref[0]
        grad = jnp.concatenate([t[0] for t in tiles], axis=1)
        right_wide = right_ref[0]
        high, low = halves(dot(left_t_ref[0], grad))
        rotated = scale * (dot(high, right_wide) + dot(low, right_wide))
        old = second_ref[0]
        new = BETA_TWO * old + (1.0 - BETA_TWO) * rotated * rotated
        second_out[0] = jnp.where(tab[base + 8 + k] == 1, new, old)
        direction = (BETA_ONE * turned_ref[0] + (1.0 - BETA_ONE) * rotated) / (
            jnp.sqrt(new) + ADAM_EPS
        )
        high, low = halves(direction)
        high, low = halves(dot(left_ref[0], high) + dot(left_ref[0], low))
        flip = ((1,), (1,))
        update = (dot(high, right_wide, flip) + dot(low, right_wide, flip)).astype(BF16)
        for j in range(per_block):
            send[:, 0, j] = update[:, j * TILE : (j + 1) * TILE].reshape(peers, rows, TILE)

    return pl.pallas_call(
        body,
        grid_spec=pltpu.PrefetchScalarGridSpec(
            num_scalar_prefetch=1,
            grid=(slots,),
            in_specs=[SMEM] + tile_specs(size, per_block, base) + [slot_spec(size)] * 5,
            out_specs=(
                slot_spec(size),
                pl.BlockSpec((peers, 1, per_block, rows, TILE), lambda k, *_: (0, k, 0, 0, 0)),
            ),
        ),
        out_shape=(
            jax.ShapeDtypeStruct((slots, size, size), F32),
            jax.ShapeDtypeStruct((peers, slots, per_block, rows, TILE), BF16),
        ),
        compiler_params=params(28),
        name="main_step",
    )(tables, factor, *([arrived] * per_block), turned, left_t, left, right, second)


def statistics(tables, factor, arrived, left_stat, right_stat, moment, base):
    slots, size, _ = left_stat.shape
    per_block = size // TILE

    def body(tab, factor_ref, *refs):
        tiles = refs[:per_block]
        left_ref, right_ref, moment_ref, left_out, right_out, moment_out = refs[per_block:]
        here = tab[base + 8 + pl.program_id(0)] == 1
        scale = factor_ref[0]
        squared = (1.0 - BETA_STAT) * (scale * scale)
        grad = jnp.concatenate([t[0] for t in tiles], axis=1)
        old = left_ref[0]
        new = BETA_STAT * old + squared * dot(grad, grad, ((1,), (1,)))
        left_out[0] = jnp.where(here, new, old)
        old = right_ref[0]
        new = BETA_STAT * old + squared * dot(grad.T, grad)
        right_out[0] = jnp.where(here, new, old)
        old = moment_ref[0]
        new = BETA_ONE * old + (1.0 - BETA_ONE) * scale * grad.astype(F32)
        moment_out[0] = jnp.where(here, new, old)

    return pl.pallas_call(
        body,
        grid_spec=pltpu.PrefetchScalarGridSpec(
            num_scalar_prefetch=1,
            grid=(slots,),
            in_specs=[SMEM] + tile_specs(size, per_block, base) + [slot_spec(size)] * 3,
            out_specs=(slot_spec(size),) * 3,
        ),
        out_shape=(jax.ShapeDtypeStruct((slots, size, size), F32),) * 3,
        compiler_params=params(28),
        name="statistics",
    )(tables, factor, *([arrived] * per_block), left_stat, right_stat, moment)


def place_tiles(tables, received, shard_tiles):
    places, rows, _ = received.shape
    tile_count = 112 if False else places // 8 * shard_tiles
    peers = tile_count // shard_tiles

    def body(tab, received_ref, out):
        def step(p, c):
            for i in range(shard_tiles):
                out[p, :, i * TILE : (i + 1) * TILE] = received_ref[tab[p * shard_tiles + i]]
            return c

        lax.fori_loop(0, peers, step, 0)

    vmem = pl.BlockSpec(memory_space=pltpu.VMEM)
    return pl.pallas_call(
        body,
        out_shape=jax.ShapeDtypeStruct((peers, rows, shard_tiles * TILE), BF16),
        in_specs=[SMEM, vmem],
        out_specs=vmem,
        compiler_params=params(6),
        name="place_tiles",
    )(tables, received)


def pull_slow(slow_flat, fast_rows, update_rows):
    peers, rows, width = fast_rows.shape

    def body(slow_ref, fast_ref, update_ref, out):
        slow = slow_ref[...]
        fast = fast_ref[0] - STEP_RATE * update_ref[0].astype(F32)
        out[...] = slow + PULL_RATE * (fast - slow)

    flat = pl.BlockSpec((rows, width), lambda p: (0, p))
    part = pl.BlockSpec((1, rows, width), lambda p: (p, 0, 0))
    return pl.pallas_call(
        body,
        grid=(peers,),
        out_shape=jax.ShapeDtypeStruct(slow_flat.shape, F32),
        in_specs=[flat, part, part],
        out_specs=flat,
        compiler_params=params(4),
        name="pull_slow",
    )(slow_flat, fast_rows, update_rows)


def exchange(x):
    return lax.all_to_all(x, TENSOR, split_axis=0, concat_axis=0, tiled=True)


def on_device(
    gradient,
    block_owner,
    tile_block,
    fast_weight,
    slow_flat,
    left_stat,
    right_stat,
    left_basis,
    right_basis,
    first_moment,
    second_moment,
):
    slots, size, _ = left_stat.shape
    row_count, shard_cols = gradient.shape
    peers = lax.axis_size(TENSOR)
    row_groups, tile_count = tile_block.shape
    shard_tiles = shard_cols // TILE
    per_block = size // TILE
    row_blocks = block_owner.shape[0] // row_groups
    total_count = row_count * shard_cols * lax.axis_size(DP) * peers

    outgoing = pack_tiles(gradient, tile_block, block_owner, peers)
    arrived = exchange(outgoing)
    tables = route_tables(tile_block, block_owner, peers, shard_tiles, row_blocks, per_block)
    wide = gradient.astype(F32)
    square_sum = functools.reduce(lax.psum, DP, jnp.sum(wide * wide))
    square_sum = exchange(jnp.full((peers, 8, TILE), square_sum, F32))
    square_sum = jnp.sum(square_sum[:, 0, 0])
    factor = (CLIP_RMS / jnp.sqrt(square_sum / total_count + 1e-06)).reshape(1)
    turned, left_t = turn_moment(left_basis, right_basis, first_moment)
    fast_rows = exchange(fast_weight.reshape(peers, row_count // peers, shard_cols))

    second_new, send = main_step(
        tables, factor, arrived, turned, left_t, left_basis, right_basis, second_moment, tile_count
    )
    received = exchange(send)
    left_new, right_new, moment_new = statistics(
        tables, factor, arrived, left_stat, right_stat, first_moment, tile_count
    )
    received = received.reshape(peers * slots * per_block, row_count // peers, TILE)
    update_rows = place_tiles(tables, received, shard_tiles)
    home = exchange(update_rows).reshape(row_count, shard_cols)
    slow_new = pull_slow(slow_flat, fast_rows, update_rows)
    fast_new = fast_weight - STEP_RATE * home.astype(F32)
    return (fast_new, slow_new, left_new, right_new, moment_new, second_new)


def solution(mesh):
    torus = Mesh(mesh.devices.reshape(4, 2, 4, 4), ("dp_0", "dp_1", "tensor_0", "tensor_1"))
    flat = P(DP_TENSOR, None)
    state = P(DP_TENSOR, None, None)
    return jax.shard_map(
        on_device,
        mesh=torus,
        in_specs=(P(DP, TENSOR), P(), P(), P(DP, TENSOR), flat) + (state,) * 6,
        out_specs=(P(DP, TENSOR), flat) + (state,) * 4,
        check_vma=False,
    )
```

```python
import functools

import jax
import jax.numpy as jnp
from jax import lax
from jax.experimental import pallas as pl
from jax.experimental.pallas import tpu as pltpu
from jax.sharding import Mesh
from jax.sharding import PartitionSpec as P


TENSOR = ("tensor_0", "tensor_1")
DP = ("dp_0", "dp_1")
DP_TENSOR = ("dp_0", "dp_1", "tensor_0", "tensor_1")

BETA_STAT = 0.95
BETA_ONE = 0.9
BETA_TWO = 0.95
ADAM_EPS = 1e-08
STEP_RATE = 0.1
PULL_RATE = 0.5
CLIP_RMS = 0.5

F32 = jnp.float32
BF16 = jnp.bfloat16
TILE = 128
SPLIT = 320
MIB = 1 << 20


def dot(a, b, dims=((1,), (0,))):
    return lax.dot_general(a, b, (dims, ((), ())), preferred_element_type=F32)


def halves(x):
    high = x.astype(BF16)
    return high, (x - high.astype(F32)).astype(BF16)


SMALL = pltpu.CompilerParams(vmem_limit_bytes=8 * MIB)
PARAMS = pltpu.CompilerParams(vmem_limit_bytes=58 * MIB)


SMEM = pl.BlockSpec(memory_space=pltpu.SMEM)
VMEM = pl.BlockSpec(memory_space=pltpu.VMEM)
HBM = pl.BlockSpec(memory_space=pltpu.HBM)


def pack_tiles(gradient, tile_block, block_owner, peers, start, rows, parts=None):
    cols = gradient.shape[1]
    tiles = cols // TILE
    extra = 0 if parts is None else 32

    def body(tb, owner, grad, *refs):
        if extra:
            parts_ref, out, tile_v, addends, in_sems, out_sems = refs
        else:
            out, tile_v, in_sems, out_sems = refs
        row = lax.axis_index(DP)
        column = lax.axis_index(TENSOR)
        loads = []
        for i in range(tiles):
            loads.append(
                pltpu.make_async_copy(
                    grad.at[pl.ds(start, rows), pl.ds(i * TILE, TILE)], tile_v.at[i], in_sems.at[i]
                )
            )
            loads[-1].start()
        stores = []

        def store(source, target, n):
            stores.append(pltpu.make_async_copy(source, target, out_sems.at[n]))
            stores[-1].start()

        if extra:
            rest = parts_ref[...]
            pieces = []
            for _ in range(3):
                piece = rest.astype(BF16).astype(F32)
                pieces.append(piece)
                rest = rest - piece
            pieces.append(jnp.zeros_like(rest))
            addends[...] = jnp.concatenate(pieces, axis=0).astype(BF16)
            for p in range(peers):
                store(addends, out.at[p, pl.ds(rows, extra)], tiles + p)
        for i in range(tiles):
            slot = owner[tb[row, column * tiles + i]]
            target = (slot >> 1) & (peers - 1)
            loads[i].wait()
            store(tile_v.at[i], out.at[target, pl.ds(0, rows)], i)
        for copy in stores:
            copy.wait()

    return pl.pallas_call(
        body,
        out_shape=jax.ShapeDtypeStruct((peers, rows + extra, TILE), BF16),
        in_specs=[SMEM, SMEM, HBM] + ([VMEM] if extra else []),
        out_specs=HBM,
        scratch_shapes=[pltpu.VMEM((tiles, rows, TILE), BF16)]
        + ([pltpu.VMEM((extra, TILE), BF16)] if extra else [])
        + [
            pltpu.SemaphoreType.DMA((tiles,)),
            pltpu.SemaphoreType.DMA((tiles + (peers if extra else 0),)),
        ],
        compiler_params=PARAMS,
        name="pack",
    )(tile_block, block_owner, gradient, *([parts] if extra else []))


def route_tables(tile_block, block_owner, tensor_size, shard_tiles, row_blocks, per_block):
    tile_count = tile_block.shape[1]

    def body(tb, owner, out, count):
        row = lax.axis_index(DP)
        mine = row * tensor_size + lax.axis_index(TENSOR)

        def clear(i, c):
            count[i] = 0
            return c

        lax.fori_loop(0, row_blocks, clear, 0)
        for i in range(tile_count, tile_count + 16):
            out[i] = 0

        def step(g, c):
            block = tb[row, g]
            local = block - row * row_blocks
            j = count[local]
            count[local] = j + 1
            slot = owner[block]
            out[g] = (((slot >> 1) & (tensor_size - 1)) * 2 + (slot & 1)) * per_block + j

            @pl.when((slot >> 1) == mine)
            def _():
                out[tile_count + (slot & 1) * per_block + j] = g // shard_tiles
                out[tile_count + 8 + (slot & 1)] = 1

            return c

        lax.fori_loop(0, tile_count, step, 0)

    return pl.pallas_call(
        body,
        out_shape=jax.ShapeDtypeStruct((128,), jnp.int32),
        in_specs=[SMEM, SMEM],
        out_specs=SMEM,
        scratch_shapes=[pltpu.SMEM((row_blocks,), jnp.int32)],
        compiler_params=PARAMS,
        name="tables",
    )(tile_block, block_owner)


def square_parts(gradient):
    def body(grad, out):
        wide = grad[...].astype(F32)
        rows, cols = wide.shape
        part = jnp.sum((wide * wide).reshape(rows // 8, 8, cols), axis=0)
        out[...] = functools.reduce(
            jnp.add, [part[:, c : c + TILE] for c in range(0, cols, TILE)]
        )

    return pl.pallas_call(
        body,
        out_shape=jax.ShapeDtypeStruct((8, TILE), F32),
        in_specs=[VMEM],
        out_specs=VMEM,
        compiler_params=PARAMS,
        name="square_parts",
    )(gradient)


def clip_factor(parts, total_count):
    total = jnp.sum(jnp.sum(parts.astype(F32), axis=0), keepdims=True)
    return CLIP_RMS / jnp.sqrt(total / total_count + 1e-06)


def slot_spec(size):
    return pl.BlockSpec((1, size, size), lambda k, *_: (k, 0, 0))


def turn_moment(left, right, moment):
    slots, size, _ = left.shape

    def body(left_ref, right_ref, moment_ref, out, flipped):
        left_t = left_ref[0].T
        flipped[0] = left_t
        high, low = halves(moment_ref[0])
        half = dot(left_t, high) + dot(left_t, low)
        high, low = halves(half)
        out[0] = dot(high, right_ref[0]) + dot(low, right_ref[0])

    return pl.pallas_call(
        body,
        grid=(slots,),
        out_shape=(
            jax.ShapeDtypeStruct((slots, size, size), F32),
            jax.ShapeDtypeStruct((slots, size, size), BF16),
        ),
        in_specs=[slot_spec(size)] * 3,
        out_specs=(slot_spec(size), slot_spec(size)),
        compiler_params=PARAMS,
        name="turn_moment",
    )(left, right, moment)


def main_step(tables, first, rest, turned, left_t, left, right, second, base, total_count):
    slots, size, _ = left.shape
    per_block = size // TILE
    peers, split, _ = first.shape
    rows = size // peers
    names = 5 + 2 * per_block

    def body(
        tab, first_ref, rest_ref, turned_ref, left_t_ref, left_ref, right_ref, second_ref,
        second_out, send_out, grad_out, scale_out,
        grad_v, left_t_v, right_v, second_v, turned_v, left_v, new_v, send_v, parts_v, sems,
        out_sems,
    ):
        def loads(k):
            pairs = [(left_t_ref.at[k], left_t_v.at[k])]
            for j in range(per_block):
                source = tab[base + k * per_block + j]
                cols = pl.ds(j * TILE, TILE)
                pairs.append((first_ref.at[source], grad_v.at[k, pl.ds(0, split), cols]))
                pairs.append(
                    (
                        rest_ref.at[source, pl.ds(0, size - split)],
                        grad_v.at[k, pl.ds(split, size - split), cols],
                    )
                )
            pairs += [
                (right_ref.at[k], right_v.at[k]),
                (second_ref.at[k], second_v.at[k]),
                (turned_ref.at[k], turned_v.at[k]),
                (left_ref.at[k], left_v.at[k]),
            ]
            return [
                pltpu.make_async_copy(a, b, sems.at[k, n]) for n, (a, b) in enumerate(pairs)
            ]

        copies = [loads(k) for k in range(slots)]
        parts_copy = pltpu.make_async_copy(
            rest_ref.at[:, pl.ds(size - split, 32)], parts_v, out_sems.at[0, 3]
        )
        parts_copy.start()
        for group in copies:
            for copy in group:
                copy.start()
        parts_copy.wait()
        scale = clip_factor(parts_v[...], total_count)
        scale_out[...] = jnp.broadcast_to(scale, scale_out.shape)
        outs = []

        def emit(source, target, k, n):
            outs.append(pltpu.make_async_copy(source, target, out_sems.at[k, n]))
            outs[-1].start()

        for k in range(slots):
            wait = copies[k]
            for copy in wait[:-4]:
                copy.wait()
            emit(grad_v.at[k], grad_out.at[k], k, 2)
            high, low = halves(dot(left_t_v[k], grad_v[k]))
            wait[-4].wait()
            right_wide = right_v[k]
            rotated = scale * (dot(high, right_wide) + dot(low, right_wide))
            wait[-3].wait()
            old = second_v[k]
            new = BETA_TWO * old + (1.0 - BETA_TWO) * rotated * rotated
            new_v[k] = jnp.where(tab[base + 8 + k] == 1, new, old)
            emit(new_v.at[k], second_out.at[k], k, 0)
            wait[-2].wait()
            direction = (BETA_ONE * turned_v[k] + (1.0 - BETA_ONE) * rotated) / (
                jnp.sqrt(new) + ADAM_EPS
            )
            high, low = halves(direction)
            wait[-1].wait()
            high, low = halves(dot(left_v[k], high) + dot(left_v[k], low))
            flip = ((1,), (1,))
            update = (dot(high, right_wide, flip) + dot(low, right_wide, flip)).astype(BF16)
            width = per_block * rows
            for j in range(per_block):
                start = k * width + j * rows
                send_v[:, start : start + rows] = update[:, j * TILE : (j + 1) * TILE].reshape(
                    peers, rows, TILE
                )
            part = pl.ds(k * width, width)
            emit(send_v.at[:, part], send_out.at[:, part], k, 1)
        for out in outs:
            out.wait()

    square = (slots, size, size)
    return pl.pallas_call(
        body,
        out_shape=(
            jax.ShapeDtypeStruct(square, F32),
            jax.ShapeDtypeStruct((peers, slots * per_block * rows, TILE), BF16),
            jax.ShapeDtypeStruct(square, BF16),
            jax.ShapeDtypeStruct((8, TILE), F32),
        ),
        in_specs=[SMEM] + [HBM] * 7,
        out_specs=(HBM, HBM, HBM, VMEM),
        scratch_shapes=[pltpu.VMEM(square, BF16)] * 3
        + [pltpu.VMEM(square, F32)] * 2
        + [pltpu.VMEM(square, BF16), pltpu.VMEM(square, F32)]
        + [
            pltpu.VMEM((peers, slots * per_block * rows, TILE), BF16),
            pltpu.VMEM((peers, 32, TILE), BF16),
            pltpu.SemaphoreType.DMA((slots, names)),
            pltpu.SemaphoreType.DMA((slots, 4)),
        ],
        compiler_params=PARAMS,
        name="main_step",
    )(tables, first, rest, turned, left_t, left, right, second)


def statistics(tables, scale, grad, left_stat, right_stat, moment, base):
    slots, size, _ = left_stat.shape

    def body(tab, scale_ref, grad_ref, left_ref, right_ref, moment_ref, *outs):
        left_out, right_out, moment_out = outs
        here = tab[base + 8 + pl.program_id(0)] == 1
        scale = scale_ref[0:1, 0:1]
        squared = (1.0 - BETA_STAT) * (scale * scale)
        grad = grad_ref[0]
        old = left_ref[0]
        new = BETA_STAT * old + squared * dot(grad, grad, ((1,), (1,)))
        left_out[0] = jnp.where(here, new, old)
        old = right_ref[0]
        new = BETA_STAT * old + squared * dot(grad.T, grad)
        right_out[0] = jnp.where(here, new, old)
        old = moment_ref[0]
        new = BETA_ONE * old + (1.0 - BETA_ONE) * scale * grad.astype(F32)
        moment_out[0] = jnp.where(here, new, old)

    return pl.pallas_call(
        body,
        grid_spec=pltpu.PrefetchScalarGridSpec(
            num_scalar_prefetch=1,
            grid=(slots,),
            in_specs=[VMEM] + [slot_spec(size)] * 4,
            out_specs=(slot_spec(size),) * 3,
        ),
        out_shape=(jax.ShapeDtypeStruct((slots, size, size), F32),) * 3,
        compiler_params=PARAMS,
        name="statistics",
    )(tables, scale, grad, left_stat, right_stat, moment)


def place_tiles(tables, received, shard_tiles):
    places, rows, _ = received.shape
    peers = places // 8

    def body(tab, received_ref, out):
        def step(p, c):
            for i in range(shard_tiles):
                out[p, :, i * TILE : (i + 1) * TILE] = received_ref[tab[p * shard_tiles + i]]
            return c

        lax.fori_loop(0, peers, step, 0)

    return pl.pallas_call(
        body,
        out_shape=jax.ShapeDtypeStruct((peers, rows, shard_tiles * TILE), BF16),
        in_specs=[SMEM, VMEM],
        out_specs=VMEM,
        compiler_params=SMALL,
        name="place_tiles",
    )(tables, received)


def pull_slow(slow_flat, fast_rows, update_rows):
    peers, rows, width = fast_rows.shape
    step = 4

    def body(slow_ref, fast_ref, update_ref, out):
        for q in range(step):
            cols = slice(q * width, (q + 1) * width)
            slow = slow_ref[:, cols]
            fast = fast_ref[q] - STEP_RATE * update_ref[q].astype(F32)
            out[:, cols] = slow + PULL_RATE * (fast - slow)

    flat = pl.BlockSpec((rows, step * width), lambda p: (0, p))
    part = pl.BlockSpec((step, rows, width), lambda p: (p, 0, 0))
    return pl.pallas_call(
        body,
        grid=(peers // step,),
        out_shape=jax.ShapeDtypeStruct(slow_flat.shape, F32),
        in_specs=[flat, part, part],
        out_specs=flat,
        compiler_params=PARAMS,
        name="pull_slow",
    )(slow_flat, fast_rows, update_rows)


def exchange(x, axes=TENSOR):
    return lax.all_to_all(x, axes, split_axis=0, concat_axis=0, tiled=True)


def on_device(
    gradient,
    block_owner,
    tile_block,
    fast_weight,
    slow_flat,
    left_stat,
    right_stat,
    left_basis,
    right_basis,
    first_moment,
    second_moment,
):
    slots, size, _ = left_stat.shape
    row_count, shard_cols = gradient.shape
    peers = lax.axis_size(TENSOR)
    row_groups, tile_count = tile_block.shape
    shard_tiles = shard_cols // TILE
    per_block = size // TILE
    row_blocks = block_owner.shape[0] // row_groups
    total_count = row_count * shard_cols * lax.axis_size(DP) * peers

    first = pack_tiles(gradient, tile_block, block_owner, peers, 0, SPLIT)
    first = exchange(first)
    parts = square_parts(gradient)
    parts = functools.reduce(lax.psum, DP, parts)
    rest = pack_tiles(gradient, tile_block, block_owner, peers, SPLIT, size - SPLIT, parts)
    rest = exchange(rest)
    tables = route_tables(tile_block, block_owner, peers, shard_tiles, row_blocks, per_block)
    turned, left_t = turn_moment(left_basis, right_basis, first_moment)
    by_rows = (peers, row_count // peers, shard_cols)
    fast_half = fast_weight.reshape(by_rows).astype(jnp.float16)
    fast_rows = exchange(fast_half)
    second_new, send, grad, scale = main_step(
        tables, first, rest, turned, left_t, left_basis, right_basis, second_moment,
        tile_count, total_count,
    )
    received = exchange(send)
    left_new, right_new, moment_new = statistics(
        tables, scale, grad, left_stat, right_stat, first_moment, tile_count
    )
    received = received.reshape(peers * slots * per_block, row_count // peers, TILE)
    update_rows = place_tiles(tables, received, shard_tiles)
    home = exchange(update_rows)
    slow_new = pull_slow(slow_flat, fast_rows.astype(F32), update_rows)
    fast_new = fast_weight.reshape(by_rows) - STEP_RATE * home.astype(F32)
    fast_new = fast_new.reshape(row_count, shard_cols)
    return (fast_new, slow_new, left_new, right_new, moment_new, second_new)


def solution(mesh):
    torus = Mesh(mesh.devices.reshape(4, 2, 4, 4), ("dp_0", "dp_1", "tensor_0", "tensor_1"))
    flat = P(DP_TENSOR, None)
    state = P(DP_TENSOR, None, None)
    return jax.shard_map(
        on_device,
        mesh=torus,
        in_specs=(P(DP, TENSOR), P(), P(), P(DP, TENSOR), flat) + (state,) * 6,
        out_specs=(P(DP, TENSOR), flat) + (state,) * 4,
        check_vma=False,
    )
```

```python
import jax
import jax.numpy as jnp
from jax import lax
from jax.experimental import pallas as pl
from jax.experimental.pallas import tpu as pltpu
from jax.sharding import Mesh
from jax.sharding import PartitionSpec as P


TENSOR = ("tensor_0", "tensor_1")
DP = ("dp_0", "dp_1")
DP_TENSOR = ("dp_0", "dp_1", "tensor_0", "tensor_1")

BETA_STAT = 0.95
BETA_ONE = 0.9
BETA_TWO = 0.95
ADAM_EPS = 1e-08
STEP_RATE = 0.1
PULL_RATE = 0.5
CLIP_RMS = 0.5

F32 = jnp.float32
BF16 = jnp.bfloat16
TILE = 128
MIB = 1 << 20


def dot(a, b, dims=((1,), (0,))):
    return lax.dot_general(a, b, (dims, ((), ())), preferred_element_type=F32)


def halves(x):
    high = x.astype(BF16)
    return high, (x - high.astype(F32)).astype(BF16)


WHOLE = pltpu.CompilerParams(vmem_limit_bytes=127 * MIB // 2)
SMALL = pltpu.CompilerParams(vmem_limit_bytes=8 * MIB)
PARAMS = pltpu.CompilerParams(vmem_limit_bytes=58 * MIB)


SMEM = pl.BlockSpec(memory_space=pltpu.SMEM)
VMEM = pl.BlockSpec(memory_space=pltpu.VMEM)
HBM = pl.BlockSpec(memory_space=pltpu.HBM)


def cut_tiles(gradient):
    peers, rows, cols = gradient.shape
    tiles = cols // TILE
    height = tiles * rows

    def body(grad, out, tile_v, in_sems, out_sems):
        loads = []
        for i in range(tiles):
            part = pl.ds(i * rows, rows)
            loads.append(
                pltpu.make_async_copy(
                    grad.at[:, :, pl.ds(i * TILE, TILE)], tile_v.at[:, part], in_sems.at[i]
                )
            )
            loads[-1].start()
        stores = []

        def store(start, size, n):
            part = pl.ds(start, size)
            stores.append(
                pltpu.make_async_copy(tile_v.at[:, part], out.at[:, part], out_sems.at[n])
            )
            stores[-1].start()

        total = jnp.zeros((8, TILE), F32)
        for i in range(tiles):
            loads[i].wait()
            store(i * rows, rows, i)
            wide = tile_v[:, i * rows : (i + 1) * rows].astype(F32)
            total = total + jnp.sum((wide * wide).reshape(-1, 8, TILE), axis=0)
        rest = jnp.sum(total, axis=0, keepdims=True)
        line = lax.broadcasted_iota(jnp.int32, (8, TILE), 0)
        lines = jnp.zeros((8, TILE), F32)
        for n in range(3):
            piece = rest.astype(BF16).astype(F32)
            lines = jnp.where(line == n, piece, lines)
            rest = rest - piece
        tile_v[:, height:] = jnp.broadcast_to(lines.astype(BF16)[None], (peers, 8, TILE))
        store(height, 8, tiles)
        for copy in stores:
            copy.wait()

    return pl.pallas_call(
        body,
        out_shape=jax.ShapeDtypeStruct((peers, height + 8, TILE), BF16),
        in_specs=[HBM],
        out_specs=HBM,
        scratch_shapes=[
            pltpu.VMEM((peers, height + 8, TILE), BF16),
            pltpu.SemaphoreType.DMA((tiles,)),
            pltpu.SemaphoreType.DMA((tiles + 1,)),
        ],
        compiler_params=PARAMS,
        name="cut_tiles",
    )(gradient)


def gather_tiles(tables, cut, places, rows):
    peers, height, _ = cut.shape
    height -= 8
    tiles = height // rows

    def body(tab, cut_ref, out, parts_out):
        parts_out[...] = jnp.sum(cut_ref[:, height:].astype(F32), axis=0)

        def step(p, c):
            for i in range(tiles):
                out[tab[p * tiles + i]] = cut_ref[p, i * rows : (i + 1) * rows]
            return c

        lax.fori_loop(0, peers, step, 0)

    return pl.pallas_call(
        body,
        out_shape=(
            jax.ShapeDtypeStruct((places, rows, TILE), BF16),
            jax.ShapeDtypeStruct((8, TILE), F32),
        ),
        in_specs=[SMEM, VMEM],
        out_specs=(VMEM, VMEM),
        compiler_params=SMALL,
        name="gather_tiles",
    )(tables, cut)


def route_tables(tile_block, block_owner, tensor_size, row_blocks, per_block):
    tile_count = tile_block.shape[1]

    def body(tb, owner, out, count):
        row = lax.axis_index(DP)
        mine = row * tensor_size + lax.axis_index(TENSOR)

        def clear(i, c):
            count[i] = 0
            return c

        lax.fori_loop(0, row_blocks, clear, 0)
        for i in range(tile_count, 128):
            out[i] = 0

        def step(g, c):
            block = tb[row, g]
            local = block - row * row_blocks
            j = count[local]
            count[local] = j + 1
            slot = owner[block]
            out[g] = (((slot >> 1) & (tensor_size - 1)) * 2 + (slot & 1)) * per_block + j

            @pl.when((slot >> 1) == mine)
            def _():
                out[tile_count + (slot & 1)] = 1

            return c

        lax.fori_loop(0, tile_count, step, 0)

    return pl.pallas_call(
        body,
        out_shape=jax.ShapeDtypeStruct((128,), jnp.int32),
        in_specs=[SMEM, SMEM],
        out_specs=SMEM,
        scratch_shapes=[pltpu.SMEM((row_blocks,), jnp.int32)],
        compiler_params=SMALL,
        name="tables",
    )(tile_block, block_owner)


def clip_factor(parts, total_count):
    total = jnp.sum(parts, keepdims=True)
    return CLIP_RMS / jnp.sqrt(total / total_count + 1e-06)


def slot_spec(size):
    return pl.BlockSpec((1, size, size), lambda k, *_: (k, 0, 0))


def turn_moment(left, right, moment):
    slots, size, _ = left.shape

    def body(left_ref, right_ref, moment_ref, out, flipped):
        left_t = left_ref[0].T
        flipped[0] = left_t
        high, low = halves(moment_ref[0])
        half = dot(left_t, high) + dot(left_t, low)
        high, low = halves(half)
        out[0] = dot(high, right_ref[0]) + dot(low, right_ref[0])

    return pl.pallas_call(
        body,
        grid=(slots,),
        out_shape=(
            jax.ShapeDtypeStruct((slots, size, size), F32),
            jax.ShapeDtypeStruct((slots, size, size), BF16),
        ),
        in_specs=[slot_spec(size)] * 3,
        out_specs=(slot_spec(size), slot_spec(size)),
        compiler_params=PARAMS,
        name="turn_moment",
    )(left, right, moment)


def main_step(tables, parts, other, arrived, turned, left_t, left, right, second, base, total_count):
    slots, size, _ = left.shape
    per_block = size // TILE
    peers = arrived.shape[0]
    rows = size // peers
    names = 5 + per_block

    def body(
        tab, parts_ref, other_ref, arrived_ref, turned_ref, left_t_ref, left_ref, right_ref, second_ref,
        second_out, send_out, grad_out, scale_out,
        grad_v, left_t_v, right_v, second_v, turned_v, left_v, new_v, send_v, sems, out_sems,
    ):
        def loads(k):
            pairs = [(left_t_ref.at[k], left_t_v.at[k])]
            for j in range(per_block):
                place = pl.ds((k * per_block + j) * rows, rows)
                cols = pl.ds(j * TILE, TILE)
                pairs.append((arrived_ref.at[:, place], grad_v.at[k, :, :, cols]))
            pairs += [
                (right_ref.at[k], right_v.at[k]),
                (second_ref.at[k], second_v.at[k]),
                (turned_ref.at[k], turned_v.at[k]),
                (left_ref.at[k], left_v.at[k]),
            ]
            return [
                pltpu.make_async_copy(a, b, sems.at[k, n]) for n, (a, b) in enumerate(pairs)
            ]

        copies = [loads(k) for k in range(slots)]
        for copy in copies[0]:
            copy.start()
        scale = clip_factor(parts_ref[...] + other_ref[...], total_count)
        scale_out[...] = jnp.broadcast_to(scale, scale_out.shape)
        outs = []

        def emit(source, target, k, n):
            outs.append(pltpu.make_async_copy(source, target, out_sems.at[k, n]))
            outs[-1].start()

        for k in range(slots):
            wait = copies[k]
            for copy in wait[:-4]:
                copy.wait()
            emit(grad_v.at[k], grad_out.at[k], k, 2)
            if k + 1 < slots:
                for copy in copies[k + 1]:
                    copy.start()
            high, low = halves(dot(left_t_v[k], grad_v[k].reshape(size, size)))
            wait[-4].wait()
            right_wide = right_v[k]
            rotated = scale * (dot(high, right_wide) + dot(low, right_wide))
            wait[-3].wait()
            old = second_v[k]
            new = BETA_TWO * old + (1.0 - BETA_TWO) * rotated * rotated
            new_v[k] = jnp.where(tab[base + k] == 1, new, old)
            emit(new_v.at[k], second_out.at[k], k, 0)
            wait[-2].wait()
            direction = (BETA_ONE * turned_v[k] + (1.0 - BETA_ONE) * rotated) / (
                jnp.sqrt(new) + ADAM_EPS
            )
            high, low = halves(direction)
            wait[-1].wait()
            high, low = halves(dot(left_v[k], high) + dot(left_v[k], low))
            flip = ((1,), (1,))
            update = (dot(high, right_wide, flip) + dot(low, right_wide, flip)).astype(BF16)
            width = per_block * rows
            for j in range(per_block):
                start = k * width + j * rows
                send_v[:, start : start + rows] = update[:, j * TILE : (j + 1) * TILE].reshape(
                    peers, rows, TILE
                )
            part = pl.ds(k * width, width)
            emit(send_v.at[:, part], send_out.at[:, part], k, 1)
        for out in outs:
            out.wait()

    square = (slots, size, size)
    return pl.pallas_call(
        body,
        out_shape=(
            jax.ShapeDtypeStruct(square, F32),
            jax.ShapeDtypeStruct((peers, slots * per_block * rows, TILE), BF16),
            jax.ShapeDtypeStruct((slots, peers, rows, size), BF16),
            jax.ShapeDtypeStruct((8, TILE), F32),
        ),
        in_specs=[SMEM, VMEM, VMEM] + [HBM] * 6,
        out_specs=(HBM, HBM, HBM, VMEM),
        scratch_shapes=[pltpu.VMEM((slots, peers, rows, size), BF16)]
        + [pltpu.VMEM(square, BF16)] * 2
        + [pltpu.VMEM(square, F32)] * 2
        + [pltpu.VMEM(square, BF16), pltpu.VMEM(square, F32)]
        + [
            pltpu.VMEM((peers, slots * per_block * rows, TILE), BF16),
            pltpu.SemaphoreType.DMA((slots, names)),
            pltpu.SemaphoreType.DMA((slots, 3)),
        ],
        compiler_params=WHOLE,
        name="main_step",
    )(tables, parts, other, arrived, turned, left_t, left, right, second)


def statistics(tables, scale, grad, left_stat, right_stat, moment, base):
    slots, size, _ = left_stat.shape

    def body(tab, scale_ref, grad_ref, left_ref, right_ref, moment_ref, *outs):
        left_out, right_out, moment_out = outs
        here = tab[base + pl.program_id(0)] == 1
        scale = scale_ref[0:1, 0:1]
        squared = (1.0 - BETA_STAT) * (scale * scale)
        grad = grad_ref[0]
        old = left_ref[0]
        new = BETA_STAT * old + squared * dot(grad, grad, ((1,), (1,)))
        left_out[0] = jnp.where(here, new, old)
        old = right_ref[0]
        new = BETA_STAT * old + squared * dot(grad.T, grad)
        right_out[0] = jnp.where(here, new, old)
        old = moment_ref[0]
        new = BETA_ONE * old + (1.0 - BETA_ONE) * scale * grad.astype(F32)
        moment_out[0] = jnp.where(here, new, old)

    return pl.pallas_call(
        body,
        grid_spec=pltpu.PrefetchScalarGridSpec(
            num_scalar_prefetch=1,
            grid=(slots,),
            in_specs=[VMEM] + [slot_spec(size)] * 4,
            out_specs=(slot_spec(size),) * 3,
        ),
        out_shape=(jax.ShapeDtypeStruct((slots, size, size), F32),) * 3,
        compiler_params=PARAMS,
        name="statistics",
    )(tables, scale, grad, left_stat, right_stat, moment)


def place_tiles(tables, received, shard_tiles):
    places, rows, _ = received.shape
    peers = places // 8

    def body(tab, received_ref, out):
        def step(p, c):
            for i in range(shard_tiles):
                out[p, :, i * TILE : (i + 1) * TILE] = received_ref[tab[p * shard_tiles + i]]
            return c

        lax.fori_loop(0, peers, step, 0)

    return pl.pallas_call(
        body,
        out_shape=jax.ShapeDtypeStruct((peers, rows, shard_tiles * TILE), BF16),
        in_specs=[SMEM, VMEM],
        out_specs=VMEM,
        compiler_params=SMALL,
        name="place_tiles",
    )(tables, received)


def pull_slow(slow_flat, fast_rows, update_rows):
    peers, rows, width = fast_rows.shape
    step = 4

    def body(slow_ref, fast_ref, update_ref, out):
        for q in range(step):
            cols = slice(q * width, (q + 1) * width)
            slow = slow_ref[:, cols]
            fast = fast_ref[q] - STEP_RATE * update_ref[q].astype(F32)
            out[:, cols] = slow + PULL_RATE * (fast - slow)

    flat = pl.BlockSpec((rows, step * width), lambda p: (0, p))
    part = pl.BlockSpec((step, rows, width), lambda p: (p, 0, 0))
    return pl.pallas_call(
        body,
        grid=(peers // step,),
        out_shape=jax.ShapeDtypeStruct(slow_flat.shape, F32),
        in_specs=[flat, part, part],
        out_specs=flat,
        compiler_params=PARAMS,
        name="pull_slow",
    )(slow_flat, fast_rows, update_rows)


def exchange(x, axes=TENSOR):
    return lax.all_to_all(x, axes, split_axis=0, concat_axis=0, tiled=True)


def on_device(
    gradient,
    block_owner,
    tile_block,
    fast_weight,
    slow_flat,
    left_stat,
    right_stat,
    left_basis,
    right_basis,
    first_moment,
    second_moment,
):
    slots, size, _ = left_stat.shape
    row_count, shard_cols = gradient.shape
    peers = lax.axis_size(TENSOR)
    row_groups, tile_count = tile_block.shape
    shard_tiles = shard_cols // TILE
    per_block = size // TILE
    row_blocks = block_owner.shape[0] // row_groups
    total_count = row_count * shard_cols * lax.axis_size(DP) * peers

    rows = row_count // peers
    places = peers * slots * per_block
    cut = exchange(cut_tiles(gradient.reshape(peers, rows, shard_cols)))
    tables = route_tables(tile_block, block_owner, peers, row_blocks, per_block)
    outgoing, parts = gather_tiles(tables, cut, places, rows)
    arrived = exchange(outgoing.reshape(peers, slots * per_block * rows, TILE))
    parts = lax.psum(parts, DP[0])
    pairs = [(i, i ^ 1) for i in range(lax.axis_size(DP[1]))]
    other = lax.ppermute(parts, DP[1], pairs)
    turned, left_t = turn_moment(left_basis, right_basis, first_moment)
    by_rows = (peers, rows, shard_cols)
    fast_half = fast_weight.reshape(by_rows).astype(jnp.float16)
    fast_rows = exchange(fast_half)
    second_new, send, grad, scale = main_step(
        tables, parts, other, arrived, turned, left_t, left_basis, right_basis, second_moment,
        tile_count, total_count,
    )
    received = exchange(send)
    fast_rows, grad = lax.optimization_barrier((fast_rows.astype(F32), grad))
    left_new, right_new, moment_new = statistics(
        tables, scale, grad.reshape(slots, size, size), left_stat, right_stat, first_moment,
        tile_count,
    )
    received = received.reshape(places, rows, TILE)
    update_rows = place_tiles(tables, received, shard_tiles)
    home = exchange(update_rows)
    slow_new = pull_slow(slow_flat, fast_rows, update_rows)
    fast_new = fast_weight.reshape(by_rows) - STEP_RATE * home.astype(F32)
    fast_new = fast_new.reshape(row_count, shard_cols)
    return (fast_new, slow_new, left_new, right_new, moment_new, second_new)


def solution(mesh):
    torus = Mesh(mesh.devices.reshape(4, 2, 4, 4), ("dp_0", "dp_1", "tensor_0", "tensor_1"))
    flat = P(DP_TENSOR, None)
    state = P(DP_TENSOR, None, None)
    return jax.shard_map(
        on_device,
        mesh=torus,
        in_specs=(P(DP, TENSOR), P(), P(), P(DP, TENSOR), flat) + (state,) * 6,
        out_specs=(P(DP, TENSOR), flat) + (state,) * 4,
        check_vma=False,
    )
```

```python
import jax
import jax.numpy as jnp
from jax import lax
from jax.experimental import pallas as pl
from jax.experimental.pallas import tpu as pltpu
from jax.sharding import Mesh
from jax.sharding import PartitionSpec as P


TENSOR = ("tensor_0", "tensor_1")
DP = ("dp_0", "dp_1")
DP_TENSOR = ("dp_0", "dp_1", "tensor_0", "tensor_1")

BETA_STAT = 0.95
BETA_ONE = 0.9
BETA_TWO = 0.95
ADAM_EPS = 1e-08
STEP_RATE = 0.1
PULL_RATE = 0.5
CLIP_RMS = 0.5

F32 = jnp.float32
BF16 = jnp.bfloat16
TILE = 128
MIB = 1 << 20


def dot(a, b, dims=((1,), (0,))):
    return lax.dot_general(a, b, (dims, ((), ())), preferred_element_type=F32)


def halves(x):
    high = x.astype(BF16)
    return high, (x - high.astype(F32)).astype(BF16)


WHOLE = pltpu.CompilerParams(vmem_limit_bytes=127 * MIB // 2)
SMALL = pltpu.CompilerParams(vmem_limit_bytes=8 * MIB)
PARAMS = pltpu.CompilerParams(vmem_limit_bytes=58 * MIB)


SMEM = pl.BlockSpec(memory_space=pltpu.SMEM)
VMEM = pl.BlockSpec(memory_space=pltpu.VMEM)
HBM = pl.BlockSpec(memory_space=pltpu.HBM)


def cut_tiles(gradient):
    peers, rows, cols = gradient.shape
    tiles = cols // TILE
    height = tiles * rows

    def body(grad, out, tile_v, in_sems, out_sems):
        loads = []
        for i in range(tiles):
            part = pl.ds(i * rows, rows)
            loads.append(
                pltpu.make_async_copy(
                    grad.at[:, :, pl.ds(i * TILE, TILE)], tile_v.at[:, part], in_sems.at[i]
                )
            )
            loads[-1].start()
        stores = []

        def store(start, size, n):
            part = pl.ds(start, size)
            stores.append(
                pltpu.make_async_copy(tile_v.at[:, part], out.at[:, part], out_sems.at[n])
            )
            stores[-1].start()

        total = jnp.zeros((8, TILE), F32)
        for i in range(tiles):
            loads[i].wait()
            store(i * rows, rows, i)
            wide = tile_v[:, i * rows : (i + 1) * rows].astype(F32)
            total = total + jnp.sum((wide * wide).reshape(-1, 8, TILE), axis=0)
        rest = jnp.sum(total, axis=0, keepdims=True)
        line = lax.broadcasted_iota(jnp.int32, (8, TILE), 0)
        lines = jnp.zeros((8, TILE), F32)
        for n in range(3):
            piece = rest.astype(BF16).astype(F32)
            lines = jnp.where(line == n, piece, lines)
            rest = rest - piece
        tile_v[:, height:] = jnp.broadcast_to(lines.astype(BF16)[None], (peers, 8, TILE))
        store(height, 8, tiles)
        for copy in stores:
            copy.wait()

    return pl.pallas_call(
        body,
        out_shape=jax.ShapeDtypeStruct((peers, height + 8, TILE), BF16),
        in_specs=[HBM],
        out_specs=HBM,
        scratch_shapes=[
            pltpu.VMEM((peers, height + 8, TILE), BF16),
            pltpu.SemaphoreType.DMA((tiles,)),
            pltpu.SemaphoreType.DMA((tiles + 1,)),
        ],
        compiler_params=PARAMS,
        name="cut_tiles",
    )(gradient)


def gather_tiles(tables, cut, places, rows):
    peers, height, _ = cut.shape
    height -= 8
    tiles = height // rows

    def body(tab, cut_ref, out, parts_out):
        parts_out[...] = jnp.sum(cut_ref[:, height:].astype(F32), axis=0)

        for p in range(peers):
            for i in range(tiles):
                out[tab[p * tiles + i]] = cut_ref[p, i * rows : (i + 1) * rows]

    return pl.pallas_call(
        body,
        out_shape=(
            jax.ShapeDtypeStruct((places, rows, TILE), BF16),
            jax.ShapeDtypeStruct((8, TILE), F32),
        ),
        in_specs=[SMEM, VMEM],
        out_specs=(VMEM, VMEM),
        compiler_params=SMALL,
        name="gather_tiles",
    )(tables, cut)


def route_tables(tile_block, block_owner, tensor_size, row_blocks, per_block):
    tile_count = tile_block.shape[1]

    def body(tb, owner, out, count):
        row = lax.axis_index(DP)
        mine = row * tensor_size + lax.axis_index(TENSOR)

        def clear(i, c):
            count[i] = 0
            return c

        lax.fori_loop(0, row_blocks, clear, 0)
        for i in range(tile_count, 128):
            out[i] = 0

        def step(g, c):
            block = tb[row, g]
            local = block - row * row_blocks
            j = count[local]
            count[local] = j + 1
            slot = owner[block]
            out[g] = (((slot >> 1) & (tensor_size - 1)) * 2 + (slot & 1)) * per_block + j

            @pl.when((slot >> 1) == mine)
            def _():
                out[tile_count + (slot & 1)] = 1

            return c

        lax.fori_loop(0, tile_count, step, 0)

    return pl.pallas_call(
        body,
        out_shape=jax.ShapeDtypeStruct((128,), jnp.int32),
        in_specs=[SMEM, SMEM],
        out_specs=SMEM,
        scratch_shapes=[pltpu.SMEM((row_blocks,), jnp.int32)],
        compiler_params=SMALL,
        name="tables",
    )(tile_block, block_owner)


def clip_factor(parts, total_count):
    total = jnp.sum(parts, keepdims=True)
    return CLIP_RMS / jnp.sqrt(total / total_count + 1e-06)


def slot_spec(size):
    return pl.BlockSpec((1, size, size), lambda k, *_: (k, 0, 0))


def turn_moment(left, right, moment):
    slots, size, _ = left.shape

    def body(left_ref, right_ref, moment_ref, out, flipped):
        left_t = left_ref[0].T
        flipped[0] = left_t
        high, low = halves(moment_ref[0])
        half = dot(left_t, high) + dot(left_t, low)
        high, low = halves(half)
        out[0] = dot(high, right_ref[0]) + dot(low, right_ref[0])

    return pl.pallas_call(
        body,
        grid=(slots,),
        out_shape=(
            jax.ShapeDtypeStruct((slots, size, size), F32),
            jax.ShapeDtypeStruct((slots, size, size), BF16),
        ),
        in_specs=[slot_spec(size)] * 3,
        out_specs=(slot_spec(size), slot_spec(size)),
        compiler_params=PARAMS,
        name="turn_moment",
    )(left, right, moment)


def main_step(tables, parts, other, arrived, turned, left_t, left, right, second, base, total_count):
    slots, size, _ = left.shape
    per_block = size // TILE
    peers = arrived.shape[0]
    rows = size // peers
    names = 5 + per_block

    def body(
        tab, parts_ref, other_ref, arrived_ref, turned_ref, left_t_ref, left_ref, right_ref, second_ref,
        second_out, send_out, grad_out, scale_out,
        grad_v, left_t_v, right_v, second_v, turned_v, left_v, new_v, send_v, sems, out_sems,
    ):
        def loads(k):
            pairs = [(left_t_ref.at[k], left_t_v.at[k])]
            for j in range(per_block):
                place = pl.ds((k * per_block + j) * rows, rows)
                cols = pl.ds(j * TILE, TILE)
                pairs.append((arrived_ref.at[:, place], grad_v.at[k, :, :, cols]))
            pairs += [
                (right_ref.at[k], right_v.at[k]),
                (second_ref.at[k], second_v.at[k]),
                (turned_ref.at[k], turned_v.at[k]),
                (left_ref.at[k], left_v.at[k]),
            ]
            return [
                pltpu.make_async_copy(a, b, sems.at[k, n]) for n, (a, b) in enumerate(pairs)
            ]

        copies = [loads(k) for k in range(slots)]
        for copy in copies[0]:
            copy.start()
        scale = clip_factor(parts_ref[...] + other_ref[...], total_count)
        scale_out[...] = jnp.broadcast_to(scale, scale_out.shape)
        outs = []

        def emit(source, target, k, n):
            outs.append(pltpu.make_async_copy(source, target, out_sems.at[k, n]))
            outs[-1].start()

        for k in range(slots):
            wait = copies[k]
            for copy in wait[:-4]:
                copy.wait()
            emit(grad_v.at[k], grad_out.at[k], k, 2)
            if k + 1 < slots:
                for copy in copies[k + 1]:
                    copy.start()
            high, low = halves(dot(left_t_v[k], grad_v[k].reshape(size, size)))
            wait[-4].wait()
            right_wide = right_v[k]
            rotated = scale * (dot(high, right_wide) + dot(low, right_wide))
            wait[-3].wait()
            old = second_v[k]
            new = BETA_TWO * old + (1.0 - BETA_TWO) * rotated * rotated
            new_v[k] = jnp.where(tab[base + k] == 1, new, old)
            emit(new_v.at[k], second_out.at[k], k, 0)
            wait[-2].wait()
            direction = (BETA_ONE * turned_v[k] + (1.0 - BETA_ONE) * rotated) / (
                jnp.sqrt(new) + ADAM_EPS
            )
            high, low = halves(direction)
            wait[-1].wait()
            high, low = halves(dot(left_v[k], high) + dot(left_v[k], low))
            flip = ((1,), (1,))
            update = (dot(high, right_wide, flip) + dot(low, right_wide, flip)).astype(BF16)
            width = per_block * rows
            for j in range(per_block):
                start = k * width + j * rows
                send_v[:, start : start + rows] = update[:, j * TILE : (j + 1) * TILE].reshape(
                    peers, rows, TILE
                )
            part = pl.ds(k * width, width)
            emit(send_v.at[:, part], send_out.at[:, part], k, 1)
        for out in outs:
            out.wait()

    square = (slots, size, size)
    return pl.pallas_call(
        body,
        out_shape=(
            jax.ShapeDtypeStruct(square, F32),
            jax.ShapeDtypeStruct((peers, slots * per_block * rows, TILE), BF16),
            jax.ShapeDtypeStruct((slots, peers, rows, size), BF16),
            jax.ShapeDtypeStruct((8, TILE), F32),
        ),
        in_specs=[SMEM, VMEM, VMEM] + [HBM] * 6,
        out_specs=(HBM, HBM, HBM, VMEM),
        scratch_shapes=[pltpu.VMEM((slots, peers, rows, size), BF16)]
        + [pltpu.VMEM(square, BF16)] * 2
        + [pltpu.VMEM(square, F32)] * 2
        + [pltpu.VMEM(square, BF16), pltpu.VMEM(square, F32)]
        + [
            pltpu.VMEM((peers, slots * per_block * rows, TILE), BF16),
            pltpu.SemaphoreType.DMA((slots, names)),
            pltpu.SemaphoreType.DMA((slots, 3)),
        ],
        compiler_params=WHOLE,
        name="main_step",
    )(tables, parts, other, arrived, turned, left_t, left, right, second)


def statistics(tables, scale, grad, left_stat, right_stat, moment, base):
    slots, size, _ = left_stat.shape

    def body(tab, scale_ref, grad_ref, left_ref, right_ref, moment_ref, *outs):
        left_out, right_out, moment_out = outs
        here = tab[base + pl.program_id(0)] == 1
        scale = scale_ref[0:1, 0:1]
        squared = (1.0 - BETA_STAT) * (scale * scale)
        grad = grad_ref[0]
        old = left_ref[0]
        new = BETA_STAT * old + squared * dot(grad, grad, ((1,), (1,)))
        left_out[0] = jnp.where(here, new, old)
        old = right_ref[0]
        new = BETA_STAT * old + squared * dot(grad.T, grad)
        right_out[0] = jnp.where(here, new, old)
        old = moment_ref[0]
        new = BETA_ONE * old + (1.0 - BETA_ONE) * scale * grad.astype(F32)
        moment_out[0] = jnp.where(here, new, old)

    return pl.pallas_call(
        body,
        grid_spec=pltpu.PrefetchScalarGridSpec(
            num_scalar_prefetch=1,
            grid=(slots,),
            in_specs=[VMEM] + [slot_spec(size)] * 4,
            out_specs=(slot_spec(size),) * 3,
        ),
        out_shape=(jax.ShapeDtypeStruct((slots, size, size), F32),) * 3,
        compiler_params=PARAMS,
        name="statistics",
    )(tables, scale, grad, left_stat, right_stat, moment)


def place_tiles(tables, received, shard_tiles):
    places, rows, _ = received.shape
    peers = places // 8
    groups = 4
    step = peers // groups
    shape = (peers, rows, shard_tiles * TILE)

    def body(tab, received_ref, out, out_v, sems):
        copies = []
        for n in range(groups):
            for p in range(n * step, (n + 1) * step):
                for i in range(shard_tiles):
                    tile = received_ref[tab[p * shard_tiles + i]]
                    out_v[p, :, i * TILE : (i + 1) * TILE] = tile
            part = pl.ds(n * step, step)
            copies.append(pltpu.make_async_copy(out_v.at[part], out.at[part], sems.at[n]))
            copies[-1].start()
        for copy in copies:
            copy.wait()

    return pl.pallas_call(
        body,
        out_shape=jax.ShapeDtypeStruct(shape, BF16),
        in_specs=[SMEM, VMEM],
        out_specs=HBM,
        scratch_shapes=[pltpu.VMEM(shape, BF16), pltpu.SemaphoreType.DMA((groups,))],
        compiler_params=SMALL,
        name="place_tiles",
    )(tables, received)


def pull_slow(slow_flat, fast_rows, update_rows):
    peers, rows, width = fast_rows.shape
    step = 4

    def body(slow_ref, fast_ref, update_ref, out):
        for q in range(step):
            cols = slice(q * width, (q + 1) * width)
            slow = slow_ref[:, cols]
            fast = fast_ref[q] - STEP_RATE * update_ref[q].astype(F32)
            out[:, cols] = slow + PULL_RATE * (fast - slow)

    flat = pl.BlockSpec((rows, step * width), lambda p: (0, p))
    part = pl.BlockSpec((step, rows, width), lambda p: (p, 0, 0))
    return pl.pallas_call(
        body,
        grid=(peers // step,),
        out_shape=jax.ShapeDtypeStruct(slow_flat.shape, F32),
        in_specs=[flat, part, part],
        out_specs=flat,
        compiler_params=PARAMS,
        name="pull_slow",
    )(slow_flat, fast_rows, update_rows)


def exchange(x, axes=TENSOR):
    return lax.all_to_all(x, axes, split_axis=0, concat_axis=0, tiled=True)


def on_device(
    gradient,
    block_owner,
    tile_block,
    fast_weight,
    slow_flat,
    left_stat,
    right_stat,
    left_basis,
    right_basis,
    first_moment,
    second_moment,
):
    slots, size, _ = left_stat.shape
    row_count, shard_cols = gradient.shape
    peers = lax.axis_size(TENSOR)
    row_groups, tile_count = tile_block.shape
    shard_tiles = shard_cols // TILE
    per_block = size // TILE
    row_blocks = block_owner.shape[0] // row_groups
    total_count = row_count * shard_cols * lax.axis_size(DP) * peers

    rows = row_count // peers
    places = peers * slots * per_block
    cut = exchange(cut_tiles(gradient.reshape(peers, rows, shard_cols)))
    tables = route_tables(tile_block, block_owner, peers, row_blocks, per_block)
    outgoing, parts = gather_tiles(tables, cut, places, rows)
    arrived = exchange(outgoing.reshape(peers, slots * per_block * rows, TILE))
    parts = lax.psum(parts, DP[0])
    pairs = [(i, i ^ 1) for i in range(lax.axis_size(DP[1]))]
    other = lax.ppermute(parts, DP[1], pairs)
    turned, left_t = turn_moment(left_basis, right_basis, first_moment)
    by_rows = (peers, rows, shard_cols)
    fast_half = fast_weight.reshape(by_rows).astype(jnp.float16)
    fast_rows = exchange(fast_half)
    second_new, send, grad, scale = main_step(
        tables, parts, other, arrived, turned, left_t, left_basis, right_basis, second_moment,
        tile_count, total_count,
    )
    received = exchange(send)
    fast_rows, grad = lax.optimization_barrier((fast_rows.astype(F32), grad))
    left_new, right_new, moment_new = statistics(
        tables, scale, grad.reshape(slots, size, size), left_stat, right_stat, first_moment,
        tile_count,
    )
    received = received.reshape(places, rows, TILE)
    update_rows = place_tiles(tables, received, shard_tiles)
    home = exchange(update_rows)
    slow_new = pull_slow(slow_flat, fast_rows, update_rows)
    fast_new = fast_weight.reshape(by_rows) - STEP_RATE * home.astype(F32)
    fast_new = fast_new.reshape(row_count, shard_cols)
    return (fast_new, slow_new, left_new, right_new, moment_new, second_new)


def solution(mesh):
    torus = Mesh(mesh.devices.reshape(4, 2, 4, 4), ("dp_0", "dp_1", "tensor_0", "tensor_1"))
    flat = P(DP_TENSOR, None)
    state = P(DP_TENSOR, None, None)
    return jax.shard_map(
        on_device,
        mesh=torus,
        in_specs=(P(DP, TENSOR), P(), P(), P(DP, TENSOR), flat) + (state,) * 6,
        out_specs=(P(DP, TENSOR), flat) + (state,) * 4,
        check_vma=False,
    )
```
